32 devices in a mesh: expert: 4 (over x, core), shard: 8 (over z, y).
Axes of the slice: x: 2, y: 2, z: 4, core: 2. Of those that a mesh axis runs over, the one named last changes fastest.
Arguments:
- train_down: float32 [16, 6400, 4096], P('expert', None, 'shard'), may hold values from -0.109375 to 0.109375
- other_down: bfloat16 [16, 6400, 4096], P('expert', None, 'shard'), may hold values from -0.0390625 to 0.0390625
- router_weight: float32 [4096, 16], P('shard', 'expert'), may hold values from -0.09375 to 0.09375
- router_gain: float32 [4096], P('shard'), may hold values from 0.25 to 1.75
Outputs:
- ready_down: bfloat16 [16, 6400, 4096], P('expert', 'shard')
- scale_down: float32 [16, 6400], P('expert', 'shard')
- serve_router: bfloat16 [4096, 16], replicated
The draws below stay inside these ranges and needn't reach their ends.
All inputs are finite; a program needn't handle non-finite values. Where the reference program divides by a largest or mean magnitude, that divisor is 1e-20 or more.
Results may differ from the reference program's by a relative error of at most 0.001.
Values may be sent and summed in bfloat16 or wider, within the bound.
A program may use at most 256 MiB of HBM per device.

```python
import jax
import jax.numpy as jnp

EXPERTS = 16
D_MODEL = 4096
D_EXPERT = 6400


def spiked(array, rng, source, target, blocks, factor):
    owner, partner = [(jnp.arange(array.shape[axis_at]) // (array.shape[axis_at] // blocks)).reshape([-1 if axis == axis_at else 1 for axis in range(array.ndim)]) for axis_at in (source, target)]
    chosen = jax.random.permutation(rng, blocks)[partner]
    strong = (owner == chosen) | (owner == (partner + blocks // 2) % blocks)
    return jnp.where(strong, factor * array, array)


def block_levels(stream_key, dims, pieces, smallest, high):
    factor_of = 1.0
    for axis_at, parts in pieces:
        draws = jax.random.uniform(jax.random.fold_in(jax.random.fold_in(stream_key, 6), axis_at), (parts,), jnp.float32, smallest / len(pieces), high / len(pieces))
        factor_of = factor_of * jnp.repeat(jnp.exp(draws), dims[axis_at] // parts).reshape((-1,) + (1,) * (len(dims) - 1 - axis_at))
    return factor_of


def noise(key, dims, width, reach, pieces=(), dtype=jnp.bfloat16):
    drawn = width * jax.random.normal(key, dims, jnp.float32)
    if pieces:
        drawn = drawn * block_levels(key, dims, pieces, -0.22, 0.18)
    return jnp.clip(drawn, -reach, reach).astype(dtype)


def noise_with(rng, dims, width, reach, pieces, heavy, dtype=jnp.bfloat16):
    values = width * jax.random.normal(rng, dims, jnp.float32)
    if pieces:
        values = values * block_levels(rng, dims, pieces, -0.22, 0.18)
    return jnp.clip(spiked(values, jax.random.fold_in(rng, 3), *heavy), -reach, reach).astype(dtype)


def setup_inputs(seed: int = 0) -> dict:
    arg_keys = jax.random.split(jax.random.key(seed), 5)
    return {
        "train_down": noise_with(arg_keys[0], (EXPERTS, D_EXPERT, D_MODEL), D_EXPERT ** -0.5, 0.109375, ((0, 4), (2, 8)), (2, 1, 8, 2.0), jnp.float32),
        "other_down": noise(arg_keys[1], (EXPERTS, D_EXPERT, D_MODEL), (D_EXPERT * 4) ** -0.5, 0.0390625, ((0, 4), (2, 8))),
        "router_weight": noise(arg_keys[2], (D_MODEL, EXPERTS), D_MODEL ** -0.5, 0.09375, ((0, 8), (1, 4)), jnp.float32),
        "router_gain": jnp.clip(1.0 + 0.15 * jax.random.normal(arg_keys[3], (D_MODEL,), jnp.float32), 0.25, 1.75),
    }


def reference(train_down, other_down, router_weight, router_gain):
    latest_down = train_down + other_down.astype(jnp.float32)
    scale_down = jnp.max(jnp.abs(latest_down), axis=2)
    ready_down = (latest_down / jnp.expand_dims(scale_down, 2)).astype(jnp.bfloat16)
    serve_router = (router_weight * router_gain[:, None]).astype(jnp.bfloat16)
    return ready_down, scale_down, serve_router
```

```python
import functools

import jax
import jax.numpy as jnp
from jax import lax
from jax.experimental import pallas as pl
from jax.experimental.pallas import tpu as pltpu
from jax.sharding import PartitionSpec as P

MESH = pl.DeviceIdType.MESH
AHEAD = 2
LANES = 128


def kernel(
    groups, shards, parts,
    train, other, router, gain,
    ready, scale_out, serve,
    tbuf, obuf, stage, lmax, rmax, gown, gmax, rparts, rflip,
    tsem, osem, own_sem, data_send, data_recv, rs_send, rs_recv, ag_send, ag_recv,
    r1_send, r1_recv, r2_send, r2_recv,
):
    me = lax.axis_index("shard")
    group = lax.axis_index("expert")
    experts = train.shape[0]
    slots, _, rows, cols = tbuf.shape
    chunks = experts * parts
    block = rows * parts

    def shard_id(k):
        return lax.rem(me + k, shards)

    def group_id(k):
        return lax.rem(group + k, groups)

    barrier = pltpu.get_barrier_semaphore()
    for k in range(1, shards):
        pl.semaphore_signal(barrier, inc=1, device_id=(group, shard_id(k)), device_id_type=MESH)
    for k in range(1, groups):
        pl.semaphore_signal(barrier, inc=1, device_id=(group_id(k), me), device_id_type=MESH)

    def place(c, d):
        return c // parts, pl.ds(pl.multiple_of(d * block + lax.rem(c, parts) * rows, 8), rows)

    def load(c, d):
        e, span = place(c, d)
        slot = lax.rem(c, slots)
        return (
            pltpu.make_async_copy(train.at[e, span], tbuf.at[slot, d], tsem.at[slot, d]),
            pltpu.make_async_copy(other.at[e, span], obuf.at[slot, d], osem.at[slot, d]),
        )

    def start_load(c):
        def one(d, _):
            for copy in load(c, d):
                copy.start()
            return 0
        lax.fori_loop(0, shards, one, 0)

    def columns_of(d):
        return pl.ds(pl.multiple_of(d * cols, LANES), cols)

    def send(src, dst, send_sem, recv_sem, peer):
        return pltpu.make_async_remote_copy(
            src_ref=src, dst_ref=dst, send_sem=send_sem, recv_sem=recv_sem,
            device_id=(group, peer), device_id_type=MESH,
        )

    def data_copy(c, d):
        e = c // parts
        span = pl.ds(pl.multiple_of(lax.rem(c, parts) * rows, 8), rows)
        return stage.at[c, d], ready.at[e, span, columns_of(me)]

    start_load(0)
    start_load(1)
    pl.semaphore_wait(barrier, shards - 1 + groups - 1)

    rparts[group, me] = router[...] * gain[...]
    for k in range(1, shards):
        send(rparts.at[group, me], rparts.at[group, me], r1_send, r1_recv, shard_id(k)).start()

    def find_max(c):
        slot = lax.rem(c, slots)

        def one(d, _):
            for copy in load(c, d):
                copy.wait()
            best = None
            for j in range(0, cols, LANES):
                at = pl.ds(j, LANES)
                now = jnp.abs(tbuf[slot, d, :, at] + obuf[slot, d, :, at].astype(jnp.float32))
                best = now if best is None else jnp.maximum(best, now)
            lmax[c, d] = jnp.max(best.T, axis=0, keepdims=True)
            return 0
        lax.fori_loop(0, shards, one, 0)

        def tell(k, _):
            peer = shard_id(k)
            send(lmax.at[c, peer], rmax.at[c, me], rs_send.at[c], rs_recv.at[c], peer).start()
            return 0
        lax.fori_loop(1, shards, tell, 0)
        rmax[c, me] = lmax[c, me]

    def merge(c):
        some = rmax.at[c, pl.ds(0, shards - 1)]
        pltpu.make_async_copy(some, some, rs_recv.at[c]).wait()
        best = rmax[c, 0]
        for d in range(1, shards):
            best = jnp.maximum(best, rmax[c, d])
        gown[c] = best
        scale_out[c] = best

        def tell(k, _):
            send(gown.at[c], gmax.at[c, me], ag_send.at[c], ag_recv.at[c], shard_id(k)).start()
            return 0
        lax.fori_loop(1, shards, tell, 0)
        gmax[c, me] = best

    def narrow(c):
        slot = lax.rem(c, slots)
        some = gmax.at[c, pl.ds(0, shards - 1)]
        pltpu.make_async_copy(some, some, ag_recv.at[c]).wait()

        def one(k, _):
            d = lax.rem(me + shards // 2 + k, shards)
            tall = jnp.broadcast_to(gmax[c, d], (LANES, rows)).T
            for j in range(0, cols, LANES):
                at = pl.ds(j, LANES)
                now = tbuf[slot, d, :, at] + obuf[slot, d, :, at].astype(jnp.float32)
                stage[c, d, :, at] = (now / tall).astype(jnp.bfloat16)
            src, dst = data_copy(c, d)

            @pl.when(d != me)
            def _():
                send(src, dst, data_send.at[d], data_recv.at[me], d).start()

            @pl.when(d == me)
            def _():
                pltpu.make_async_copy(src, dst, own_sem).start()
            return 0
        lax.fori_loop(0, shards, one, 0)

    def step(c, _):
        @pl.when(c < chunks)
        def _():
            find_max(c)

        @pl.when((c >= 1) & (c <= chunks))
        def _():
            merge(c - 1)

        @pl.when(c >= AHEAD)
        def _():
            narrow(c - AHEAD)

        @pl.when(c + 2 < chunks)
        def _():
            start_load(c + 2)
        return 0

    lax.fori_loop(0, chunks + AHEAD, step, 0)

    some = rparts.at[0, pl.ds(0, shards - 1)]
    pltpu.make_async_copy(some, some, r1_recv).wait()
    for k in range(1, groups):
        pltpu.make_async_remote_copy(
            src_ref=rparts.at[group], dst_ref=rparts.at[group], send_sem=r2_send, recv_sem=r2_recv,
            device_id=(group_id(k), me), device_id_type=MESH,
        ).start()
    some = rparts.at[pl.ds(0, groups - 1)]
    pltpu.make_async_copy(some, some, r2_recv).wait()
    wide = router.shape[1]
    for d in range(shards):
        for g in range(groups):
            rflip[g * experts:(g + 1) * experts, :] = rparts[g, d]
        serve[d * wide:(d + 1) * wide, :] = rflip[...].T.astype(jnp.bfloat16)

    some = rparts.at[0, pl.ds(0, shards - 1)]
    pltpu.make_async_copy(some, some, r1_send).wait()
    some = rparts.at[pl.ds(0, groups - 1)]
    pltpu.make_async_copy(some, some, r2_send).wait()

    def drain(c, _):
        some = rmax.at[c, pl.ds(0, shards - 1)]
        pltpu.make_async_copy(some, some, rs_send.at[c]).wait()
        pltpu.make_async_copy(some, some, ag_send.at[c]).wait()
        return 0
    lax.fori_loop(0, chunks, drain, 0)

    mine = ready.at[:, :, columns_of(me)]
    pltpu.make_async_copy(mine, mine, own_sem).wait()

    def finish(k, _):
        d = shard_id(k)
        there = ready.at[:, :, columns_of(d)]
        pltpu.make_async_copy(there, there, data_send.at[d]).wait()
        pltpu.make_async_copy(there, there, data_recv.at[d]).wait()
        return 0
    lax.fori_loop(1, shards, finish, 0)


def pieces(block):
    for count in (5, 4, 3, 2):
        if block % (16 * count) == 0:
            return count
    return 1


def per_device(groups, shards, train_down, other_down, router_weight, router_gain):
    experts, height, cols = train_down.shape
    block = height // shards
    parts = pieces(block)
    rows = block // parts
    chunks = experts * parts
    slots = AHEAD + 2
    wide = router_weight.shape[0]
    f32, bf16 = jnp.float32, jnp.bfloat16
    dma = pltpu.SemaphoreType.DMA
    hbm = pl.BlockSpec(memory_space=pl.ANY)
    vmem = pl.BlockSpec(memory_space=pltpu.VMEM)
    ready, scale, serve = pl.pallas_call(
        functools.partial(kernel, groups, shards, parts),
        out_shape=(
            jax.ShapeDtypeStruct((experts, block, cols * shards), bf16),
            jax.ShapeDtypeStruct((chunks, 1, rows), f32),
            jax.ShapeDtypeStruct((wide * shards, experts * groups), bf16),
        ),
        in_specs=[hbm, hbm, vmem, vmem],
        out_specs=(hbm, vmem, vmem),
        scratch_shapes=[
            pltpu.VMEM((slots, shards, rows, cols), f32),
            pltpu.VMEM((slots, shards, rows, cols), bf16),
            pltpu.VMEM((chunks, shards, rows, cols), bf16),
            pltpu.VMEM((chunks, shards, 1, rows), f32),
            pltpu.VMEM((chunks, shards, 1, rows), f32),
            pltpu.VMEM((chunks, 1, rows), f32),
            pltpu.VMEM((chunks, shards, 1, rows), f32),
            pltpu.VMEM((groups, shards, experts, wide), f32),
            pltpu.VMEM((groups * experts, wide), f32),
            dma((slots, shards)), dma((slots, shards)), dma(()),
            dma((shards,)), dma((shards,)),
            dma((chunks,)), dma((chunks,)), dma((chunks,)), dma((chunks,)),
            dma(()), dma(()), dma(()), dma(()),
        ],
        compiler_params=pltpu.CompilerParams(
            collective_id=0, has_side_effects=True, vmem_limit_bytes=62 * 2**20
        ),
    )(train_down, other_down, router_weight.T, router_gain[None, :])
    return ready, scale.reshape(experts, block), serve


def solution(mesh):
    in_specs = (
        P("expert", None, "shard"),
        P("expert", None, "shard"),
        P("shard", "expert"),
        P("shard"),
    )
    out_specs = (P("expert", "shard", None), P("expert", "shard"), P())
    body = functools.partial(per_device, mesh.shape["expert"], mesh.shape["shard"])
    return jax.shard_map(
        body, mesh=mesh, in_specs=in_specs, out_specs=out_specs, check_vma=False
    )
```
